32 devices in a mesh: narrow: 4 (over x, core), wide: 8 (over z, y).
Axes of the slice: x: 2, y: 2, z: 4, core: 2. Of those that a mesh axis runs over, the one named last changes fastest.
Arguments:
- block_ids: int32 [512, 4], P(('narrow', 'wide')), may hold values from 0 to 511, as said below
- incidence: int32 [512, 4, 128, 128], P(('narrow', 'wide')), may hold values from 0 to 1
- costs: int32 [512, 128], P(('narrow', 'wide')), may hold values from 16 to 80
- start_mult: float32 [512, 128], replicated, may hold values from 0.25 to 4
- upper: float32 [1], replicated, may hold values from 65536 to 131072
Outputs:
- multipliers: float32 [512, 128], replicated
- primal_mean: float32 [512, 128], P(('narrow', 'wide'))
The draws below stay inside these ranges and needn't reach their ends.
Inputs may be any that keep to these rules, and one draw needn't show every extreme that they name: `block_ids`: the 4 row blocks listed for one tile are distinct.
All inputs are finite; a program needn't handle non-finite values.
Results may differ from the reference program's by a relative error of at most 0.0003.
Values sent between devices are 32-bit elements; how exact they have to be, the bound alone decides.
A program may use at most 64 MiB of HBM per device.

```python
import math
import jax
import jax.numpy as jnp
from jax import lax

BLK = 128
TILE = 128
K = 4
TILES_DEV = 16
ITERS = 3
RB = 512
TILES = 512


def pick_blocks(key):
    random_part = jax.random.randint(jax.random.fold_in(key, 17), (TILES, RB), 0, 4096)
    ranking = random_part * RB + jnp.arange(RB, dtype=jnp.int32)[None, :]
    _, chosen = lax.top_k(ranking, K)
    return chosen.astype(jnp.int32)


def draw_block_ids(key, part):
    return pick_blocks(key)


def draw_incidence(key, part):
    chosen = pick_blocks(key)
    levels = jax.random.randint(jax.random.fold_in(key, 29), (RB, BLK), 1, 9)
    row_level = jnp.take(levels, chosen, axis=0)
    entries = jax.random.randint(jax.random.fold_in(key, 31), (TILES, K, BLK, TILE), 0, K * BLK // 2)
    return (entries < row_level[:, :, :, None]).astype(jnp.int32)


def touch_ends(values, rng, low, top_value):
    spot = [jax.random.randint(jax.random.fold_in(rng, axis), (), 0, length) for axis, length in enumerate(values.shape)]
    longest = values.shape.index(max(values.shape))
    beside = spot[:longest] + [(spot[longest] + 1) % values.shape[longest]] + spot[longest + 1:]
    return values.at[tuple(spot)].set(low).at[tuple(beside)].set(top_value)


def setup_inputs(seed: int = 0) -> dict:
    key_list = jax.random.split(jax.random.key(seed), 6)
    return {
        "block_ids": draw_block_ids(jax.random.fold_in(key_list[5], 71), 0),
        "incidence": draw_incidence(jax.random.fold_in(key_list[5], 71), 0),
        "costs": touch_ends(jax.random.randint(key_list[2], (TILES, TILE), 16, 81), jax.random.fold_in(key_list[2], 1), 16, 80).astype(jnp.int32),
        "start_mult": jnp.clip(jnp.exp(jax.random.uniform(key_list[3], (RB, BLK), jnp.float32, math.log(0.25), math.log(4.0))), 0.25, 4.0),
        "upper": jnp.clip(jax.random.uniform(key_list[4], (1,), jnp.float32, 65536.0, 131072.0), 65536.0, 131072.0),
    }


def reference(block_ids, incidence, costs, start_mult, upper):
    groups = TILES // TILES_DEV
    ids_g = block_ids.reshape(groups, TILES_DEV, K)
    inc_g = incidence.reshape(groups, TILES_DEV, K, BLK, TILE)
    cost_g = costs.reshape(groups, TILES_DEV, TILE).astype(jnp.float32)
    mult = start_mult
    primal_mean = jnp.zeros((groups, TILES_DEV, TILE), jnp.float32)
    hi = lax.Precision.HIGHEST
    for step in range(ITERS):
        def reduce_cols(args):
            ids, inc, cost = args
            u_tile = jnp.take(mult, ids, axis=0)
            incf = inc.astype(jnp.float32)
            return cost - jnp.einsum('tkrc,tkr->tc', incf, u_tile, precision=hi)

        reduced = lax.map(reduce_cols, (ids_g, inc_g, cost_g))
        primal = 1.0 / (1.0 + jnp.exp(reduced / 8.0))
        soft = jnp.sum(-8.0 * jax.nn.softplus(-reduced / 8.0))
        value = jnp.sum(mult) + soft
        if step == 0:
            primal_mean = primal
        else:
            primal_mean = 0.3 * primal + 0.7 * primal_mean

        def add_cover(total, args):
            ids, inc, pm = args
            incf = inc.astype(jnp.float32)
            part = jnp.einsum('tkrc,tc->tkr', incf, pm, precision=hi).reshape(TILES_DEV * K, BLK)
            onehot = (ids.reshape(TILES_DEV * K, 1) == jnp.arange(RB, dtype=jnp.int32)[None, :]).astype(jnp.float32)
            return total + jnp.dot(onehot.T, part, precision=hi, preferred_element_type=jnp.float32), None

        cover, _ = lax.scan(add_cover, jnp.zeros((RB, BLK), jnp.float32), (ids_g, inc_g, primal_mean))
        slope = 1.0 - cover
        norm = jnp.sum(slope * slope)
        size = (upper[0] - value) / (norm + 1e-6)
        mult = jnp.maximum(0.0, mult + size * slope)
    return mult, primal_mean.reshape(TILES, TILE)
```

```python
import functools

import jax
import jax.numpy as jnp
from jax import lax
from jax.experimental import pallas as pl
from jax.experimental.pallas import tpu as pltpu
from jax.sharding import PartitionSpec as P

ITERS = 3
MESH = pl.DeviceIdType.MESH


def pieces(x):
    hi = x.astype(jnp.bfloat16)
    rest = x - hi.astype(jnp.float32)
    mid = rest.astype(jnp.bfloat16)
    lo = (rest - mid.astype(jnp.float32)).astype(jnp.bfloat16)
    return jnp.concatenate([hi, mid, lo], axis=0)


def fold(x):
    rows = x.shape[0] // 3
    return x[:rows] + x[rows : 2 * rows] + x[2 * rows :]


def kernel(
    narrow, wide, ids, inc, costs, start, upper,
    mult_out, mean_out,
    inc_buf, w, u, onehot, outgoing, incoming, share_src, cover, soft_src, soft_buf,
    load_sem, rs_send, rs_recv, ag_send, ag_recv, soft_send, soft_recv,
):
    n = narrow * wide
    tiles, k_count, blk, cols = inc.shape
    share = cover.shape[1]
    blocks = n * share
    pairs = tiles // 2
    depth = k_count * blk
    me = lax.axis_index("narrow") * wide + lax.axis_index("wide")
    unroll = n <= 32

    def device(d):
        return (d // wide, d % wide)

    def to_others(act):
        def one(i, carry):
            act((me + i) % n)
            return carry

        if unroll:
            for i in range(1, n):
                one(i, 0)
        else:
            lax.fori_loop(1, n, one, 0)

    def wait_all(ref, sem):
        part = ref.at[pl.ds(0, n - 1)]
        pltpu.make_async_copy(part, part, sem).wait()

    loads = []
    for p in range(pairs):
        copy = pltpu.make_async_copy(
            inc.at[pl.ds(2 * p, 2)], inc_buf.at[pl.ds(2 * p, 2)], load_sem.at[p]
        )
        copy.start()
        loads.append(copy)

    barrier = pltpu.get_barrier_semaphore()
    to_others(lambda d: pl.semaphore_signal(barrier, inc=1, device_id=device(d), device_id_type=MESH))

    u[...] = start[...]
    count = tiles * k_count
    lane = lax.broadcasted_iota(jnp.int32, (1, 3 * count), 1) % count
    listed = jnp.zeros((1, 3 * count), jnp.int32)
    for t in range(tiles):
        for k in range(k_count):
            listed = jnp.where(lane == k * tiles + t, ids[t, k], listed)
    row = lax.broadcasted_iota(jnp.int32, (blocks, 3 * count), 0)
    onehot[...] = (row == listed).astype(jnp.float32).astype(jnp.bfloat16)

    costf = costs[...].astype(jnp.float32)
    tile_row = lax.broadcasted_iota(jnp.int32, (tiles, cols), 0)
    tile_row_wide = lax.broadcasted_iota(jnp.int32, (tiles, depth), 0)
    mean = None
    for step in range(ITERS):
        rows = []
        for t in range(tiles):
            cells = []
            for k in range(k_count):
                b = ids[t, k]
                cells.append(u[b // share, pl.ds(b % share, 1), :])
            rows.append(jnp.concatenate(cells, axis=1))
        lhs = pieces(jnp.concatenate(rows, axis=0))
        total = jnp.zeros((tiles, cols), jnp.float32)
        for p in range(pairs):
            if step == 0:
                loads[p].wait()
                for half in range(2):
                    w[p, :, half * cols : (half + 1) * cols] = (
                        inc_buf[2 * p + half].reshape(depth, cols).astype(jnp.float32).astype(jnp.bfloat16)
                    )
            got = fold(jnp.dot(lhs, w[p], preferred_element_type=jnp.float32))
            total = jnp.where(tile_row == 2 * p, got[:, :cols], total)
            total = jnp.where(tile_row == 2 * p + 1, got[:, cols:], total)
        reduced = costf - total
        scaled = reduced * 0.125
        primal = 1.0 / (1.0 + jnp.exp(scaled))
        soft = -8.0 * (jnp.maximum(-scaled, 0.0) + jnp.log1p(jnp.exp(-jnp.abs(scaled))))
        soft_row = jnp.sum(soft, axis=0, keepdims=True)
        soft_src[step] = soft_row
        soft_buf[step, me] = soft_row
        if step == 0:
            pl.semaphore_wait(barrier, n - 1)
        to_others(
            lambda d: pltpu.make_async_remote_copy(
                src_ref=soft_src.at[step], dst_ref=soft_buf.at[step, me],
                send_sem=soft_send.at[step], recv_sem=soft_recv.at[step],
                device_id=device(d), device_id_type=MESH,
            ).start()
        )
        mean = primal if step == 0 else 0.3 * primal + 0.7 * mean
        even = tile_row % 2 == 0
        lhs = pieces(
            jnp.concatenate([jnp.where(even, mean, 0.0), jnp.where(even, 0.0, mean)], axis=1)
        )
        part = jnp.zeros((tiles, depth), jnp.float32)
        for p in range(pairs):
            got = fold(
                lax.dot_general(
                    lhs, w[p], (((1,), (1,)), ((), ())), preferred_element_type=jnp.float32
                )
            )
            part = jnp.where(tile_row_wide // 2 == p, got, part)
        part = jnp.concatenate([part[:, k * blk : (k + 1) * blk] for k in range(k_count)], axis=0)
        mine = jnp.dot(onehot[...], pieces(part), preferred_element_type=jnp.float32)
        if step > 0:
            wait_all(outgoing, rs_send)
        outgoing[...] = mine.reshape(n, share, blk)
        to_others(
            lambda d: pltpu.make_async_remote_copy(
                src_ref=outgoing.at[d], dst_ref=incoming.at[me],
                send_sem=rs_send, recv_sem=rs_recv,
                device_id=device(d), device_id_type=MESH,
            ).start()
        )
        if step > 0:
            wait_all(cover, ag_send)
        incoming[me] = outgoing[me]
        wait_all(incoming, rs_recv)
        owned = jnp.sum(incoming[...], axis=0)
        share_src[...] = owned
        cover[me] = owned
        to_others(
            lambda d: pltpu.make_async_remote_copy(
                src_ref=share_src, dst_ref=cover.at[me],
                send_sem=ag_send, recv_sem=ag_recv,
                device_id=device(d), device_id_type=MESH,
            ).start()
        )
        wait_all(soft_buf.at[step], soft_recv.at[step])
        value = jnp.sum(u[...]) + jnp.sum(soft_buf[step])
        wait_all(cover, ag_recv)
        slope = 1.0 - cover[...]
        norm = jnp.sum(slope * slope)
        size = (jnp.full((1, 1, blk), upper[0] - value)) / (norm + 1e-06)
        new = jnp.maximum(0.0, u[...] + size * slope)
        if step < ITERS - 1:
            u[...] = new
        else:
            mult_out[...] = new
            mean_out[...] = mean
    wait_all(outgoing, rs_send)
    wait_all(cover, ag_send)
    for step in range(ITERS):
        wait_all(soft_buf.at[step], soft_send.at[step])


def local(narrow, wide, block_ids, incidence, costs, start_mult, upper):
    n = narrow * wide
    tiles, k_count, blk, cols = incidence.shape
    blocks = start_mult.shape[0]
    share = blocks // n
    vmem = pl.BlockSpec(memory_space=pltpu.VMEM)
    smem = pl.BlockSpec(memory_space=pltpu.SMEM)
    rows = (n, share, blk)
    mult, mean = pl.pallas_call(
        functools.partial(kernel, narrow, wide),
        name="volume",
        out_shape=(
            jax.ShapeDtypeStruct(rows, jnp.float32),
            jax.ShapeDtypeStruct(costs.shape, jnp.float32),
        ),
        in_specs=[smem, pl.BlockSpec(memory_space=pl.ANY), vmem, vmem, smem],
        out_specs=(vmem, vmem),
        scratch_shapes=[
            pltpu.VMEM(incidence.shape, jnp.int32),
            pltpu.VMEM((tiles // 2, k_count * blk, 2 * cols), jnp.bfloat16),
            pltpu.VMEM(rows, jnp.float32),
            pltpu.VMEM((blocks, 3 * tiles * k_count), jnp.bfloat16),
            pltpu.VMEM(rows, jnp.float32),
            pltpu.VMEM(rows, jnp.float32),
            pltpu.VMEM(rows[1:], jnp.float32),
            pltpu.VMEM(rows, jnp.float32),
            pltpu.VMEM((ITERS, 1, cols), jnp.float32),
            pltpu.VMEM((ITERS, n, 1, cols), jnp.float32),
            pltpu.SemaphoreType.DMA((tiles // 2,)),
            pltpu.SemaphoreType.DMA,
            pltpu.SemaphoreType.DMA,
            pltpu.SemaphoreType.DMA,
            pltpu.SemaphoreType.DMA,
            pltpu.SemaphoreType.DMA((ITERS,)),
            pltpu.SemaphoreType.DMA((ITERS,)),
        ],
        compiler_params=pltpu.CompilerParams(collective_id=0, has_side_effects=True),
    )(block_ids, incidence, costs, start_mult.reshape(rows), upper)
    return mult.reshape(blocks, blk), mean


def solution(mesh):
    in_specs = (
        P(("narrow", "wide"), None),
        P(("narrow", "wide"), None, None, None),
        P(("narrow", "wide"), None),
        P(),
        P(),
    )
    out_specs = (P(), P(("narrow", "wide"), None))
    body = functools.partial(local, mesh.shape["narrow"], mesh.shape["wide"])
    return jax.shard_map(body, mesh=mesh, in_specs=in_specs, out_specs=out_specs, check_vma=False)
```

```python
import functools

import jax
import jax.numpy as jnp
from jax import lax
from jax.experimental import pallas as pl
from jax.experimental.pallas import tpu as pltpu
from jax.sharding import PartitionSpec as P

ITERS = 3
MESH = pl.DeviceIdType.MESH


def pieces(x):
    hi = x.astype(jnp.bfloat16)
    rest = x - hi.astype(jnp.float32)
    mid = rest.astype(jnp.bfloat16)
    lo = (rest - mid.astype(jnp.float32)).astype(jnp.bfloat16)
    return jnp.concatenate([hi, mid, lo], axis=0)


def fold(x):
    rows = x.shape[0] // 3
    return x[:rows] + x[rows : 2 * rows] + x[2 * rows :]


def kernel(
    narrow, wide, ids, inc, costs, start, upper,
    mult_out, mean_out,
    inc_buf, w, u, onehot, other_onehot, outgoing, incoming, cover,
    part_src, part_other, list_src, list_other, soft_src, soft_buf,
    load_sem, rs_send, rs_recv, ag_send, ag_recv, soft_send, soft_recv, pair_send, pair_recv,
):
    tiles, k_count, blk, cols = inc.shape
    share = cover.shape[1]
    chips = narrow * wide // 2
    half = chips * share
    pairs = tiles // 2
    depth = k_count * blk
    count = tiles * k_count
    across, along = lax.axis_index("narrow"), lax.axis_index("wide")
    core = across % 2
    me = (across // 2) * wide + along
    partner = (across + 1 - 2 * core, along)
    base = core * chips
    other_base = chips - base

    def to_others(act):
        def one(i, carry):
            d = (me + i) % chips
            act(d, ((d // wide) * 2 + core, d % wide))
            return carry

        if chips <= 16:
            for i in range(1, chips):
                one(i, 0)
        else:
            lax.fori_loop(1, chips, one, 0)

    def wait_all(ref, sem):
        part = ref.at[pl.ds(0, chips - 1)]
        pltpu.make_async_copy(part, part, sem).wait()

    def to_partner(src, dst, i):
        return pltpu.make_async_remote_copy(
            src_ref=src, dst_ref=dst, send_sem=pair_send.at[i], recv_sem=pair_recv.at[i],
            device_id=partner, device_id_type=MESH,
        )

    loads = []
    for p in range(pairs):
        copy = pltpu.make_async_copy(
            inc.at[pl.ds(2 * p, 2)], inc_buf.at[pl.ds(2 * p, 2)], load_sem.at[p]
        )
        copy.start()
        loads.append(copy)

    barrier = pltpu.get_barrier_semaphore()
    pl.semaphore_signal(barrier, inc=1, device_id=partner, device_id_type=MESH)
    to_others(
        lambda d, where: pl.semaphore_signal(barrier, inc=1, device_id=where, device_id_type=MESH)
    )

    u[...] = start[...]
    lane = lax.broadcasted_iota(jnp.int32, list_src.shape, 1) % count
    listed = jnp.zeros(list_src.shape, jnp.int32)
    for t in range(tiles):
        for k in range(k_count):
            listed = jnp.where(lane == k * tiles + t, ids[k, t], listed)
    listed = listed.astype(jnp.float32)
    list_src[...] = listed
    row = (lax.broadcasted_iota(jnp.int32, onehot.shape, 0) + core * half).astype(jnp.float32)

    def mark(names):
        return (row == names[:, : 3 * count]).astype(jnp.float32).astype(jnp.bfloat16)

    onehot[...] = mark(listed)

    costf = costs[...].astype(jnp.float32)
    tile_row = lax.broadcasted_iota(jnp.int32, (tiles, cols), 0)
    tile_row_wide = lax.broadcasted_iota(jnp.int32, (tiles, depth), 0)
    part_src[...] = jnp.zeros_like(part_src)
    share_list = to_partner(list_src, list_other, 0)
    share_part = to_partner(part_src, part_other, 1)
    own_half = cover.at[pl.ds(base, chips)]
    share_half = to_partner(own_half, own_half, 2)
    mean = None
    for step in range(ITERS):
        rows = []
        for t in range(tiles):
            cells = []
            for k in range(k_count):
                b = ids[k, t]
                cells.append(u[b // share, pl.ds(b % share, 1), :])
            rows.append(jnp.concatenate(cells, axis=1))
        lhs = pieces(jnp.concatenate(rows, axis=0))
        total = jnp.zeros((tiles, cols), jnp.float32)
        for p in range(pairs):
            if step == 0:
                loads[p].wait()
                for side in range(2):
                    w[p, :, side * cols : (side + 1) * cols] = (
                        inc_buf[2 * p + side].reshape(depth, cols).astype(jnp.float32).astype(jnp.bfloat16)
                    )
            got = fold(jnp.dot(lhs, w[p], preferred_element_type=jnp.float32))
            total = jnp.where(tile_row == 2 * p, got[:, :cols], total)
            total = jnp.where(tile_row == 2 * p + 1, got[:, cols:], total)
        if step == 0:
            pl.semaphore_wait(barrier, chips)
            share_list.start()
        reduced = costf - total
        scaled = reduced * 0.125
        primal = 1.0 / (1.0 + jnp.exp(scaled))
        mean = primal if step == 0 else 0.3 * primal + 0.7 * mean
        even = tile_row % 2 == 0
        lhs = pieces(
            jnp.concatenate([jnp.where(even, mean, 0.0), jnp.where(even, 0.0, mean)], axis=1)
        )
        part = jnp.zeros((tiles, depth), jnp.float32)
        for p in range(pairs):
            got = fold(
                lax.dot_general(
                    lhs, w[p], (((1,), (1,)), ((), ())), preferred_element_type=jnp.float32
                )
            )
            part = jnp.where(tile_row_wide // 2 == p, got, part)
        part = jnp.concatenate([part[:, k * blk : (k + 1) * blk] for k in range(k_count)], axis=0)
        soft = -8.0 * (jnp.maximum(-scaled, 0.0) + jnp.log1p(jnp.exp(-jnp.abs(scaled))))
        soft_row = jnp.sum(soft, axis=0, keepdims=True)
        if step > 0:
            share_part.wait_send()
        part_src[:count] = part
        part_src[count : count + 1] = soft_row
        share_part.start()
        if step > 0:
            wait_all(outgoing, rs_send)
            wait_all(cover, ag_send)
            share_half.wait_send()
        mine = jnp.dot(onehot[...], pieces(part), preferred_element_type=jnp.float32)
        if step == 0:
            share_list.wait_recv()
            other_onehot[...] = mark(list_other[...])
        share_part.wait_recv()
        mine = mine + jnp.dot(
            other_onehot[...], pieces(part_other[:count]), preferred_element_type=jnp.float32
        )
        outgoing[...] = mine.reshape(chips, share, blk)
        to_others(
            lambda d, where: pltpu.make_async_remote_copy(
                src_ref=outgoing.at[d], dst_ref=incoming.at[me],
                send_sem=rs_send, recv_sem=rs_recv,
                device_id=where, device_id_type=MESH,
            ).start()
        )
        soft_row = soft_row + part_other[count : count + 1]
        soft_src[step] = soft_row
        soft_buf[step, me] = soft_row
        to_others(
            lambda d, where: pltpu.make_async_remote_copy(
                src_ref=soft_src.at[step], dst_ref=soft_buf.at[step, me],
                send_sem=soft_send.at[step], recv_sem=soft_recv.at[step],
                device_id=where, device_id_type=MESH,
            ).start()
        )
        incoming[me] = outgoing[me]
        mult_sum = jnp.sum(u[...])
        wait_all(incoming, rs_recv)
        cover[base + me] = jnp.sum(incoming[...], axis=0)
        to_others(
            lambda d, where: pltpu.make_async_remote_copy(
                src_ref=cover.at[base + me], dst_ref=cover.at[base + me],
                send_sem=ag_send, recv_sem=ag_recv,
                device_id=where, device_id_type=MESH,
            ).start()
        )
        wait_all(soft_buf.at[step], soft_recv.at[step])
        value = mult_sum + jnp.sum(soft_buf[step])
        wait_all(cover, ag_recv)
        share_half.start()
        slope = 1.0 - cover[pl.ds(base, chips)]
        norm = jnp.sum(slope * slope)
        share_half.wait_recv()
        slope = 1.0 - cover[pl.ds(other_base, chips)]
        norm = norm + jnp.sum(slope * slope)
        size = (jnp.full((1, 1, blk), upper[0] - value)) / (norm + 1e-06)
        new = jnp.maximum(0.0, u[...] + size * (1.0 - cover[...]))
        if step < ITERS - 1:
            u[...] = new
        else:
            mult_out[...] = new
            mean_out[...] = mean
    wait_all(outgoing, rs_send)
    wait_all(cover, ag_send)
    for step in range(ITERS):
        wait_all(soft_buf.at[step], soft_send.at[step])
    share_list.wait_send()
    share_part.wait_send()
    share_half.wait_send()


def local(narrow, wide, block_ids, incidence, costs, start_mult, upper):
    n = narrow * wide
    tiles, k_count, blk, cols = incidence.shape
    blocks = start_mult.shape[0]
    share = blocks // n
    count = tiles * k_count
    f32 = jnp.float32
    vmem = pl.BlockSpec(memory_space=pltpu.VMEM)
    smem = pl.BlockSpec(memory_space=pltpu.SMEM)
    rows = (n, share, blk)
    half = (n // 2, share, blk)
    dma = pltpu.SemaphoreType.DMA
    mult, mean = pl.pallas_call(
        functools.partial(kernel, narrow, wide),
        name="volume",
        out_shape=(
            jax.ShapeDtypeStruct(rows, f32),
            jax.ShapeDtypeStruct(costs.shape, f32),
        ),
        in_specs=[smem, pl.BlockSpec(memory_space=pltpu.HBM), vmem, vmem, smem],
        out_specs=(vmem, vmem),
        scratch_shapes=[
            pltpu.VMEM(incidence.shape, jnp.int32),
            pltpu.VMEM((tiles // 2, k_count * blk, 2 * cols), jnp.bfloat16),
            pltpu.VMEM(rows, f32),
            pltpu.VMEM((blocks // 2, 3 * count), jnp.bfloat16),
            pltpu.VMEM((blocks // 2, 3 * count), jnp.bfloat16),
            pltpu.VMEM(half, f32),
            pltpu.VMEM(half, f32),
            pltpu.VMEM(rows, f32),
            pltpu.VMEM((count + 8, blk), f32),
            pltpu.VMEM((count + 8, blk), f32),
            pltpu.VMEM((1, 4 * count), f32),
            pltpu.VMEM((1, 4 * count), f32),
            pltpu.VMEM((ITERS, 1, cols), f32),
            pltpu.VMEM((ITERS, n // 2, 1, cols), f32),
            dma((tiles // 2,)), dma, dma, dma, dma, dma((ITERS,)), dma((ITERS,)), dma((3,)), dma((3,)),
        ],
        compiler_params=pltpu.CompilerParams(
            collective_id=0, has_side_effects=True, vmem_limit_bytes=52 * 2**20
        ),
    )(block_ids.T, incidence, costs, start_mult.reshape(rows), upper)
    return mult.reshape(blocks, blk), mean


def solution(mesh):
    in_specs = (
        P(("narrow", "wide"), None),
        P(("narrow", "wide"), None, None, None),
        P(("narrow", "wide"), None),
        P(),
        P(),
    )
    out_specs = (P(), P(("narrow", "wide"), None))
    body = functools.partial(local, mesh.shape["narrow"], mesh.shape["wide"])
    return jax.shard_map(body, mesh=mesh, in_specs=in_specs, out_specs=out_specs, check_vma=False)
```

```python
import functools

import jax
import jax.numpy as jnp
from jax import lax
from jax.experimental import pallas as pl
from jax.experimental.pallas import tpu as pltpu
from jax.sharding import PartitionSpec as P

ITERS = 3
MESH = pl.DeviceIdType.MESH


def pieces(x):
    hi = x.astype(jnp.bfloat16)
    rest = x - hi.astype(jnp.float32)
    mid = rest.astype(jnp.bfloat16)
    lo = (rest - mid.astype(jnp.float32)).astype(jnp.bfloat16)
    return jnp.concatenate([hi, mid, lo], axis=0)


def fold(x):
    rows = x.shape[0] // 3
    return x[:rows] + x[rows : 2 * rows] + x[2 * rows :]


def kernel(
    narrow, wide, ids, inc, costs, start, upper,
    mult_out, mean_out,
    inc_buf, w, u, onehot, other_onehot, outgoing, incoming, cover,
    part_src, part_other, list_src, list_other, soft_src, soft_buf,
    load_sem, rs_send, rs_recv, ag_send, ag_recv, soft_send, soft_recv, pair_send, pair_recv,
):
    tiles, k_count, blk, cols = inc.shape
    share = cover.shape[1]
    chips = narrow * wide // 2
    half = chips * share
    pairs = tiles // 2
    depth = k_count * blk
    count = tiles * k_count
    across, along = lax.axis_index("narrow"), lax.axis_index("wide")
    core = across % 2
    me = (across // 2) * wide + along
    partner = (across + 1 - 2 * core, along)
    base = core * chips
    other_base = chips - base

    def to_others(act):
        def go(d):
            act(d, ((d // wide) * 2 + core, d % wide))

        def one(i, carry):
            go((me + i) % chips)
            return carry

        if chips <= 16 and chips & (chips - 1) == 0:
            for i in sorted(range(1, chips), key=lambda i: -i.bit_count()):
                d = me
                for bit in range(chips.bit_length() - 1):
                    if (i >> bit) & 1:
                        d = d + (1 << bit) * (1 - 2 * ((me // (1 << bit)) % 2))
                go(d)
        else:
            lax.fori_loop(1, chips, one, 0)

    def wait_all(ref, sem):
        part = ref.at[pl.ds(0, chips - 1)]
        pltpu.make_async_copy(part, part, sem).wait()

    def to_partner(src, dst, i):
        return pltpu.make_async_remote_copy(
            src_ref=src, dst_ref=dst, send_sem=pair_send.at[i], recv_sem=pair_recv.at[i],
            device_id=partner, device_id_type=MESH,
        )

    loads = []
    for p in range(pairs):
        copy = pltpu.make_async_copy(
            inc.at[pl.ds(2 * p, 2)], inc_buf.at[pl.ds(2 * p, 2)], load_sem.at[p]
        )
        copy.start()
        loads.append(copy)

    barrier = pltpu.get_barrier_semaphore()
    pl.semaphore_signal(barrier, inc=1, device_id=partner, device_id_type=MESH)
    to_others(
        lambda d, where: pl.semaphore_signal(barrier, inc=1, device_id=where, device_id_type=MESH)
    )

    u[...] = start[...]
    lane = lax.broadcasted_iota(jnp.int32, list_src.shape, 1) % count
    listed = jnp.zeros(list_src.shape, jnp.int32)
    for t in range(tiles):
        for k in range(k_count):
            listed = jnp.where(lane == k * tiles + t, ids[k, t], listed)
    listed = listed.astype(jnp.float32)
    list_src[...] = listed
    row = (lax.broadcasted_iota(jnp.int32, onehot.shape, 0) + core * half).astype(jnp.float32)

    def mark(names):
        return (row == names[:, : 3 * count]).astype(jnp.float32).astype(jnp.bfloat16)

    onehot[...] = mark(listed)

    costf = costs[...].astype(jnp.float32)
    tile_row = lax.broadcasted_iota(jnp.int32, (tiles, cols), 0)
    tile_row_wide = lax.broadcasted_iota(jnp.int32, (tiles, depth), 0)
    part_src[...] = jnp.zeros_like(part_src)
    share_list = to_partner(list_src, list_other, 0)
    share_part = to_partner(part_src, part_other, 1)
    own_half = cover.at[pl.ds(base, chips)]
    share_half = to_partner(own_half, own_half, 2)
    mean = None
    for step in range(ITERS):
        rows = []
        for t in range(tiles):
            cells = []
            for k in range(k_count):
                b = ids[k, t]
                cells.append(u[b // share, pl.ds(b % share, 1), :])
            rows.append(jnp.concatenate(cells, axis=1))
        lhs = pieces(jnp.concatenate(rows, axis=0))
        total = jnp.zeros((tiles, cols), jnp.float32)
        for p in range(pairs):
            if step == 0:
                loads[p].wait()
                for side in range(2):
                    w[p, :, side * cols : (side + 1) * cols] = (
                        inc_buf[2 * p + side].reshape(depth, cols).astype(jnp.float32).astype(jnp.bfloat16)
                    )
            got = fold(jnp.dot(lhs, w[p], preferred_element_type=jnp.float32))
            total = jnp.where(tile_row == 2 * p, got[:, :cols], total)
            total = jnp.where(tile_row == 2 * p + 1, got[:, cols:], total)
        if step == 0:
            pl.semaphore_wait(barrier, chips)
            share_list.start()
        reduced = costf - total
        scaled = reduced * 0.125
        primal = 1.0 / (1.0 + jnp.exp(scaled))
        mean = primal if step == 0 else 0.3 * primal + 0.7 * mean
        even = tile_row % 2 == 0
        lhs = pieces(
            jnp.concatenate([jnp.where(even, mean, 0.0), jnp.where(even, 0.0, mean)], axis=1)
        )
        part = jnp.zeros((tiles, depth), jnp.float32)
        for p in range(pairs):
            got = fold(
                lax.dot_general(
                    lhs, w[p], (((1,), (1,)), ((), ())), preferred_element_type=jnp.float32
                )
            )
            part = jnp.where(tile_row_wide // 2 == p, got, part)
        part = jnp.concatenate([part[:, k * blk : (k + 1) * blk] for k in range(k_count)], axis=0)
        soft = -8.0 * (jnp.maximum(-scaled, 0.0) + jnp.log1p(jnp.exp(-jnp.abs(scaled))))
        soft_row = jnp.sum(soft, axis=0, keepdims=True)
        if step > 0:
            share_part.wait_send()
        part_src[:count] = part
        part_src[count : count + 1] = soft_row
        share_part.start()
        if step > 0:
            wait_all(outgoing, rs_send)
            wait_all(cover, ag_send)
            share_half.wait_send()
        mine = jnp.dot(onehot[...], pieces(part), preferred_element_type=jnp.float32)
        if step == 0:
            share_list.wait_recv()
            other_onehot[...] = mark(list_other[...])
        share_part.wait_recv()
        mine = mine + jnp.dot(
            other_onehot[...], pieces(part_other[:count]), preferred_element_type=jnp.float32
        )
        outgoing[...] = mine.reshape(chips, share, blk)
        to_others(
            lambda d, where: pltpu.make_async_remote_copy(
                src_ref=outgoing.at[d], dst_ref=incoming.at[me],
                send_sem=rs_send, recv_sem=rs_recv,
                device_id=where, device_id_type=MESH,
            ).start()
        )
        soft_row = soft_row + part_other[count : count + 1]
        soft_src[step] = soft_row
        soft_buf[step, me] = soft_row
        to_others(
            lambda d, where: pltpu.make_async_remote_copy(
                src_ref=soft_src.at[step], dst_ref=soft_buf.at[step, me],
                send_sem=soft_send.at[step], recv_sem=soft_recv.at[step],
                device_id=where, device_id_type=MESH,
            ).start()
        )
        incoming[me] = outgoing[me]
        mult_sum = jnp.sum(u[...])
        wait_all(incoming, rs_recv)
        cover[base + me] = jnp.sum(incoming[...], axis=0)
        to_others(
            lambda d, where: pltpu.make_async_remote_copy(
                src_ref=cover.at[base + me], dst_ref=cover.at[base + me],
                send_sem=ag_send, recv_sem=ag_recv,
                device_id=where, device_id_type=MESH,
            ).start()
        )
        wait_all(soft_buf.at[step], soft_recv.at[step])
        value = mult_sum + jnp.sum(soft_buf[step])
        wait_all(cover, ag_recv)
        share_half.start()
        slope = 1.0 - cover[pl.ds(base, chips)]
        norm = jnp.sum(slope * slope)
        share_half.wait_recv()
        slope = 1.0 - cover[pl.ds(other_base, chips)]
        norm = norm + jnp.sum(slope * slope)
        size = (jnp.full((1, 1, blk), upper[0] - value)) / (norm + 1e-06)
        new = jnp.maximum(0.0, u[...] + size * (1.0 - cover[...]))
        if step < ITERS - 1:
            u[...] = new
        else:
            mult_out[...] = new
            mean_out[...] = mean
    wait_all(outgoing, rs_send)
    wait_all(cover, ag_send)
    for step in range(ITERS):
        wait_all(soft_buf.at[step], soft_send.at[step])
    share_list.wait_send()
    share_part.wait_send()
    share_half.wait_send()


def local(narrow, wide, block_ids, incidence, costs, start_mult, upper):
    n = narrow * wide
    tiles, k_count, blk, cols = incidence.shape
    blocks = start_mult.shape[0]
    share = blocks // n
    count = tiles * k_count
    f32 = jnp.float32
    vmem = pl.BlockSpec(memory_space=pltpu.VMEM)
    smem = pl.BlockSpec(memory_space=pltpu.SMEM)
    rows = (n, share, blk)
    half = (n // 2, share, blk)
    dma = pltpu.SemaphoreType.DMA
    mult, mean = pl.pallas_call(
        functools.partial(kernel, narrow, wide),
        name="volume",
        out_shape=(
            jax.ShapeDtypeStruct(rows, f32),
            jax.ShapeDtypeStruct(costs.shape, f32),
        ),
        in_specs=[smem, pl.BlockSpec(memory_space=pltpu.HBM), vmem, vmem, smem],
        out_specs=(vmem, vmem),
        scratch_shapes=[
            pltpu.VMEM(incidence.shape, jnp.int32),
            pltpu.VMEM((tiles // 2, k_count * blk, 2 * cols), jnp.bfloat16),
            pltpu.VMEM(rows, f32),
            pltpu.VMEM((blocks // 2, 3 * count), jnp.bfloat16),
            pltpu.VMEM((blocks // 2, 3 * count), jnp.bfloat16),
            pltpu.VMEM(half, f32),
            pltpu.VMEM(half, f32),
            pltpu.VMEM(rows, f32),
            pltpu.VMEM((count + 8, blk), f32),
            pltpu.VMEM((count + 8, blk), f32),
            pltpu.VMEM((1, 4 * count), f32),
            pltpu.VMEM((1, 4 * count), f32),
            pltpu.VMEM((ITERS, 1, cols), f32),
            pltpu.VMEM((ITERS, n // 2, 1, cols), f32),
            dma((tiles // 2,)), dma, dma, dma, dma, dma((ITERS,)), dma((ITERS,)), dma((3,)), dma((3,)),
        ],
        compiler_params=pltpu.CompilerParams(
            collective_id=0, has_side_effects=True, vmem_limit_bytes=52 * 2**20
        ),
    )(block_ids.T, incidence, costs, start_mult.reshape(rows), upper)
    return mult.reshape(blocks, blk), mean


def solution(mesh):
    in_specs = (
        P(("narrow", "wide"), None),
        P(("narrow", "wide"), None, None, None),
        P(("narrow", "wide"), None),
        P(),
        P(),
    )
    out_specs = (P(), P(("narrow", "wide"), None))
    body = functools.partial(local, mesh.shape["narrow"], mesh.shape["wide"])
    return jax.shard_map(body, mesh=mesh, in_specs=in_specs, out_specs=out_specs, check_vma=False)
```
